32 devices in a mesh: rep: 4 (over x, y), dp: 8 (over z, core).
Axes of the slice: x: 2, y: 2, z: 4, core: 2. Of those that a mesh axis runs over, the one named last changes fastest.
Arguments:
- g_w_gate: bfloat16 [32, 2, 1280, 3072], P(('rep', 'dp')), parts along dimension 0
- g_w_up: bfloat16 [32, 2, 1280, 3072], P(('rep', 'dp')), parts along dimension 0
- g_w_down: bfloat16 [32, 2, 3072, 1280], P(('rep', 'dp')), parts along dimension 0
- w_gate: bfloat16 [2, 1280, 3072], replicated
- w_up: bfloat16 [2, 1280, 3072], replicated
- w_down: bfloat16 [2, 3072, 1280], replicated
- m_w_gate: float32 [2, 1280, 3072], P(None, 'dp')
- m_w_up: float32 [2, 1280, 3072], P(None, 'dp')
- m_w_down: float32 [2, 3072, 1280], P(None, 'dp')
- v_w_gate: float32 [2, 1280, 3072], P(None, 'dp')
- v_w_up: float32 [2, 1280, 3072], P(None, 'dp')
- v_w_down: float32 [2, 3072, 1280], P(None, 'dp')
Outputs:
- output 1: bfloat16 [8, 1280, 3072], P('rep'), parts along dimension 0
- output 2: bfloat16 [8, 1280, 3072], P('rep'), parts along dimension 0
- output 3: bfloat16 [8, 3072, 1280], P('rep'), parts along dimension 0
- output 4: float32 [8, 1280, 3072], P('rep', 'dp'), parts along dimension 0
- output 5: float32 [8, 1280, 3072], P('rep', 'dp'), parts along dimension 0
- output 6: float32 [8, 3072, 1280], P('rep', 'dp'), parts along dimension 0
- output 7: float32 [8, 1280, 3072], P('rep', 'dp'), parts along dimension 0
- output 8: float32 [8, 1280, 3072], P('rep', 'dp'), parts along dimension 0
- output 9: float32 [8, 3072, 1280], P('rep', 'dp'), parts along dimension 0
There are 4 independent parts. The reference program is written for one: setup_inputs(seed, part) draws one part's arguments, and reference() takes and returns one part's arrays. A program takes and returns all parts, laid end to end along the dimension named above; an argument that names none is the same for every part.
All inputs are finite; a program needn't handle non-finite values.
Results may differ from the reference program's by a relative error of at most 0.022.
Values are sent between devices in bfloat16 or wider.
A program may use at most 2 GiB of HBM per device.

```python
import jax
import jax.numpy as jnp
from jax import lax

DEVICES = 8
D = 1280
FF = 3072
LAYERS = 2
NAMES = ("w_gate", "w_up", "w_down")
SHAPES = {"w_gate": (LAYERS, D, FF), "w_up": (LAYERS, D, FF), "w_down": (LAYERS, FF, D)}


def setup_inputs(seed: int = 0, part: int = 0) -> dict:
    kz, *keys = jax.random.split(jax.random.key(seed), 1 + 5 * len(NAMES))
    loud = 2.0 ** jax.random.uniform(kz, (), jnp.float32, -1.0, 1.0)
    drawn = {}
    for name, key, both in zip(NAMES, keys[:3], keys[3:6], strict=True):
        own = jax.random.normal(jax.random.fold_in(key, part), (DEVICES, *SHAPES[name]), jnp.float32)
        shared = jax.random.normal(jax.random.fold_in(both, part), SHAPES[name], jnp.float32)
        drawn["g_" + name] = (loud * (0.7 * shared / DEVICES + 0.7 * own * DEVICES**-0.5)).astype(jnp.bfloat16)
    for name, key in zip(NAMES, keys[6:9], strict=True):
        drawn[name] = (jax.random.normal(key, SHAPES[name], jnp.float32) * SHAPES[name][1] ** -0.5).astype(jnp.bfloat16)
    for name, key in zip(NAMES, keys[9:12], strict=True):
        drawn["m_" + name] = loud * 0.5 * jax.random.normal(key, SHAPES[name], jnp.float32)
    for name, key in zip(NAMES, keys[12:15], strict=True):
        drawn["v_" + name] = loud * loud * jax.random.uniform(key, SHAPES[name], jnp.float32, 0.5, 1.5)
    return drawn


def adamw(w, m, v, g):
    m = 0.9 * m + 0.1 * g
    v = 0.95 * v + 0.05 * g * g
    step = m * lax.rsqrt(v + 1e-8) + 0.1 * w
    return (w - 0.02 * step).astype(jnp.bfloat16), m, v


def clipped(gradients, sum_of_squares, count):
    factor = jnp.minimum(1.0, 0.5 * lax.rsqrt(sum_of_squares / count + 1e-30))
    return [g * factor for g in gradients]


def reference(g_w_gate, g_w_up, g_w_down, w_gate, w_up, w_down, m_w_gate, m_w_up, m_w_down, v_w_gate, v_w_up, v_w_down):
    def total(terms):
        return lax.scan(lambda so_far, term: (so_far + term.astype(jnp.float32), None), jnp.zeros(terms.shape[1:], jnp.float32), terms)[0]

    gradients = [total(terms).astype(jnp.bfloat16).astype(jnp.float32) for terms in (g_w_gate, g_w_up, g_w_down)]
    gradients = clipped(gradients, sum(jnp.sum(g * g) for g in gradients), sum(g.size for g in gradients))
    new = [
        adamw(w.astype(jnp.float32), m, v, g)
        for w, m, v, g in zip((w_gate, w_up, w_down), (m_w_gate, m_w_up, m_w_down), (v_w_gate, v_w_up, v_w_down), gradients, strict=True)
    ]
    return tuple(one[which] for which in range(3) for one in new)
```

```python
import jax
import jax.numpy as jnp
from jax import lax
from jax.experimental import pallas as pl
from jax.experimental.pallas import tpu as pltpu
from jax.sharding import PartitionSpec as P

MESH = pl.DeviceIdType.MESH
CHIPS = 4
LAYERS = 2
RS_ROWS = (16, 16, 32)
AG_ROWS = (16, 16, 32)
LAG = 2
AHEAD = 3
READ = 2


def kernel(count, *refs):
    g, w, m, v = (refs[i : i + 3] for i in (0, 3, 6, 9))
    new_w, new_m, new_v = (refs[i : i + 3] for i in (12, 15, 18))
    (land_0, land_1, land_2, peer_0, peer_1, peer_2, own_a, own_b, m_a, m_b, v_a, v_b, w_a, w_b, mo_a, mo_b, vo_a, vo_b) = refs[21:39]
    (squares_a, squares_b, part, norms) = refs[39:43]
    (own_sem, peer_send, peer_recv, sum_send, sum_recv, norm_send, norm_recv, tile_sem, out_sem, g_recv, e_recv, i_recv, f_recv, o_recv) = refs[43:57]
    (send_sem, core_send, core_recv, local_sem) = refs[57:]
    land, peer = (land_0, land_1, land_2), (peer_0, peer_1, peer_2)
    own, m_in, v_in, w_in = (own_a, own_a, own_b), (m_a, m_a, m_b), (v_a, v_a, v_b), (w_a, w_a, w_b)
    m_out, v_out, squares = (mo_a, mo_a, mo_b), (vo_a, vo_a, vo_b), (squares_a, squares_a, squares_b)
    block = [ref.shape[1] for ref in land]
    f32 = jnp.float32

    me = lax.axis_index("dp")
    z, c = lax.div(me, 2), lax.rem(me, 2)
    is_end = (z == 0) | (z == 3)
    is_inner = jnp.logical_not(is_end)
    centre = jnp.where(z == 0, 1, jnp.where(z == 3, 2, 3 - z))
    outer = jnp.where(z <= 1, 0, 3)

    def core(chip):
        return {"dp": chip * 2 + c}

    other_core = {"dp": z * 2 + 1 - c}

    def remote(src, dst, send, recv, device):
        return pltpu.make_async_remote_copy(src_ref=src, dst_ref=dst, send_sem=send, recv_sem=recv, device_id=device, device_id_type=MESH)

    barrier = pltpu.get_barrier_semaphore()
    for d in range(1, 8):
        pl.semaphore_signal(barrier, inc=1, device_id={"dp": lax.rem(me + d, 8)}, device_id_type=MESH)
    pl.semaphore_wait(barrier, 7)

    def unit_of(j, layer, chip):
        return layer * CHIPS + chip

    def push_terms(j, layer, chip):
        u = unit_of(j, layer, chip)
        rows = pl.ds(pl.multiple_of((chip * 2 + 1 - c) * block[j], block[j]), block[j])
        return remote(g[j].at[layer, rows], peer[j].at[u], peer_send.at[j], peer_recv.at[j * 8 + u], other_core)

    for j in range(3):
        for layer in range(LAYERS):
            for o in range(2):
                push_terms(j, layer, o).start()
                push_terms(j, layer, 2 + o).start()

    rs_n = [block[j] // RS_ROWS[j] for j in range(3)]
    rs_k = [LAYERS * 2 * n for n in rs_n]
    rs_total = sum(rs_k)
    ag_n = [block[j] // AG_ROWS[j] for j in range(3)]
    ag_k = [LAYERS * n for n in ag_n]
    ag_total = sum(ag_k)

    def each(counts, k, body):
        first = 0
        for j in range(3):
            last = first + counts[j]

            @pl.when((k >= first) & (k < last))
            def _(j=j, first=first):
                body(j, k - first)

            first = last

    def rs_piece(flow, j, k):
        unit, s = lax.div(k, rs_n[j]), lax.rem(k, rs_n[j])
        layer, chip = lax.div(unit, 2), lax.rem(unit, 2) + 2 * flow
        return layer, chip, s

    def rows_of(j, device, s, n):
        return pl.ds(pl.multiple_of(device * block[j] + s * n, n), n)

    def load_terms(flow, j, k, slot):
        layer, chip, s = rs_piece(flow, j, k)
        rows = rows_of(j, chip * 2 + c, s, RS_ROWS[j])
        return pltpu.make_async_copy(g[j].at[layer, rows], own[j].at[flow, slot], own_sem.at[flow, slot])

    for ref in (squares_a, squares_b):
        ref[...] = jnp.zeros_like(ref)

    def sum_step(flow, i):
        source, sink = (3, 0) if flow == 0 else (0, 3)
        lag = (3 - z if flow == 0 else z) * LAG
        to = z - 1 if flow == 0 else z + 1
        k = i - lag
        each(rs_k, k + AHEAD, lambda j, q: load_terms(flow, j, q, lax.rem(k + AHEAD, AHEAD + 1)).start())

        def body(j, q):
            layer, chip, s = rs_piece(flow, j, q)
            u, n, slot = unit_of(j, layer, chip), RS_ROWS[j], lax.rem(k, AHEAD + 1)
            rows = pl.ds(pl.multiple_of(s * n, n), n)
            here = land[j].at[u, rows]
            load_terms(flow, j, q, slot).wait()

            @pl.when(s == 0)
            def _():
                remote(peer[j].at[u], peer[j].at[u], peer_send.at[j], peer_recv.at[j * 8 + u], other_core).wait_recv()

            copy = remote(here, here, sum_send.at[flow, j], sum_recv.at[flow, k], core(jnp.clip(to, 0, 3)))

            @pl.when(z != source)
            def _():
                copy.wait_recv()

            def add(fed, last):
                for r in range(0, n, 16):
                    at = pl.ds(pl.multiple_of(s * n + r, 16), 16)
                    total = own[j][flow, slot, pl.ds(r, 16)].astype(f32) + peer[j][u, at].astype(f32)
                    if fed:
                        total = land[j][u, at].astype(f32) + total
                    total = total.astype(jnp.bfloat16)
                    land[j][u, at] = total
                    if last:
                        total = total.astype(f32)
                        total = total * total
                        squares[j][...] += total[:8] + total[8:]

            @pl.when(z == source)
            def _():
                add(False, False)

            @pl.when((z != source) & (z != sink))
            def _():
                add(True, False)

            @pl.when(z == sink)
            def _():
                add(True, True)

            @pl.when(z != sink)
            def _():
                copy.start()

        each(rs_k, k, body)

    def both(i, carry):
        sum_step(0, i - AHEAD)
        sum_step(1, i - AHEAD)
        return carry

    def ag_piece(j, k):
        layer, s = lax.div(k, ag_n[j]), lax.rem(k, ag_n[j])
        return layer, s

    def tiles(j, k, slot):
        layer, s = ag_piece(j, k)
        n = AG_ROWS[j]
        rows = pl.ds(pl.multiple_of(s * n, n), n)
        return (
            pltpu.make_async_copy(m[j].at[layer, rows], m_in[j].at[slot], tile_sem.at[0, slot]),
            pltpu.make_async_copy(v[j].at[layer, rows], v_in[j].at[slot], tile_sem.at[1, slot]),
            pltpu.make_async_copy(w[j].at[layer, rows_of(j, me, s, n)], w_in[j].at[slot], tile_sem.at[2, slot]),
        )

    def start_tiles(k):
        def body(j, q):
            for copy in tiles(j, q, lax.rem(k, READ + 1)):
                copy.start()

        each(ag_k, k, body)

    for k in range(READ):
        for copy in tiles(0, k, k):
            copy.start()

    lax.fori_loop(0, rs_total + AHEAD + 3 * LAG, both, 0)

    place = jnp.where(z == 0, c, 2 + c)

    def norm_copy(d):
        return remote(part, norms.at[place], norm_send.at[d - 1], norm_recv.at[place], {"dp": lax.rem(me + d, 8)})

    @pl.when(is_end)
    def _():
        total = jnp.sum(squares_a[...]) + jnp.sum(squares_b[...])
        part[...] = jnp.full(part.shape, total, f32)
        norms[place] = jnp.full(part.shape, total, f32)
        for d in range(1, 8):
            norm_copy(d).start()

    for p in range(4):

        @pl.when(is_inner | (place != p))
        def _():
            remote(part, norms.at[p], norm_send.at[0], norm_recv.at[p], other_core).wait_recv()

    total = norms[0] + norms[1] + norms[2] + norms[3]
    factor = jnp.minimum(1.0, 0.5 * lax.rsqrt(total / count + 1e-30))[:1, :1]

    def new_piece(j, k, chip):
        layer, s = ag_piece(j, k)
        return new_w[j].at[layer, rows_of(j, chip * 2 + c, s, AG_ROWS[j])]

    def share(j, ref):
        remote(ref, ref, core_send.at[j], core_recv.at[j], other_core).start()

    def moments_out(j, k, slot):
        layer, s = ag_piece(j, k)
        n = AG_ROWS[j]
        rows = pl.ds(pl.multiple_of(s * n, n), n)
        return (
            pltpu.make_async_copy(m_out[j].at[slot], new_m[j].at[layer, rows], out_sem.at[0, slot]),
            pltpu.make_async_copy(v_out[j].at[slot], new_v[j].at[layer, rows], out_sem.at[1, slot]),
        )

    def wait_moments(k):
        def body(j, q):
            for copy in moments_out(j, q, lax.rem(k, 2)):
                copy.wait()

        each(ag_k, k, body)

    def own_step(k):
        def body(j, q):
            start_tiles(k + READ)
            wait_moments(k - 2)
            layer, s = ag_piece(j, q)
            n, slot, out = AG_ROWS[j], lax.rem(k, READ + 1), lax.rem(k, 2)
            rows = pl.ds(pl.multiple_of(s * n, n), n)
            u_own, u_new = unit_of(j, layer, z), unit_of(j, layer, lax.bitwise_xor(z, 1))
            u_handed = unit_of(j, layer, centre)

            @pl.when(is_end)
            def _():
                remote(land[j].at[u_handed, rows], peer[j].at[u_handed, rows], send_sem.at[0, j], g_recv.at[k], core(centre)).start()

            for copy in tiles(j, q, slot):
                copy.wait()

            @pl.when(is_inner)
            def _():
                remote(land[j].at[u_own, rows], peer[j].at[u_own, rows], send_sem.at[0, j], g_recv.at[k], core(centre)).wait_recv()

            def update(sums):
                for r in range(0, n, 16):
                    at, tile = pl.ds(pl.multiple_of(s * n + r, 16), 16), pl.ds(r, 16)
                    clipped = sums[j][u_own, at].astype(f32) * factor
                    one_m = 0.9 * m_in[j][slot, tile] + 0.1 * clipped
                    one_v = 0.95 * v_in[j][slot, tile] + 0.05 * clipped * clipped
                    one_w = w_in[j][slot, tile].astype(f32)
                    step = one_m * lax.rsqrt(one_v + 1e-8) + 0.1 * one_w
                    m_out[j][out, tile] = one_m
                    v_out[j][out, tile] = one_v
                    peer[j][u_new, at] = (one_w - 0.02 * step).astype(jnp.bfloat16)

            @pl.when(is_end)
            def _():
                update(land)

            @pl.when(is_inner)
            def _():
                update(peer)

            for copy in moments_out(j, q, out):
                copy.start()
            ready, there = peer[j].at[u_new, rows], new_piece(j, q, z)

            @pl.when(is_end)
            def _():
                remote(ready, there, send_sem.at[1, j], e_recv.at[k], core(centre)).start()

            @pl.when(is_inner)
            def _():
                remote(ready, there, send_sem.at[0, j], i_recv.at[k], core(outer)).start()
                remote(ready, there, send_sem.at[1, j], i_recv.at[k], core(centre)).start()

            remote(ready, there, core_send.at[j], core_recv.at[j], other_core).start()
            pltpu.make_async_copy(ready, there, local_sem.at[j]).start()

        each(ag_k, k, body)

    def arrived(k, chip, recv, forward=None):
        def body(j, q):
            ref = new_piece(j, q, chip)
            remote(ref, ref, core_send.at[j], recv.at[k], other_core).wait_recv()
            if forward is not None:
                sem, to = forward
                remote(ref, ref, send_sem.at[sem, j], f_recv.at[k], core(to)).start()
            share(j, ref)

        each(ag_k, k, body)

    near, far = jnp.where(z <= 1, 1, 2), 3 - outer

    def new_step(i, carry):
        @pl.when(is_end)
        def _():
            own_step(i)
            arrived(i - 2 * LAG, near, i_recv)
            arrived(i - 3 * LAG, far, f_recv)

        @pl.when(is_inner)
        def _():
            arrived(i - 2 * LAG, far, f_recv, (3, outer))
            arrived(i - LAG, outer, e_recv, (2, centre))
            own_step(i - LAG)
            arrived(i - 2 * LAG, centre, i_recv)

        return carry

    lax.fori_loop(0, ag_total + 3 * LAG, new_step, 0)

    def last_piece(j, layer, chip):
        return new_w[j].at[layer, pl.ds(pl.multiple_of((chip * 2 + c) * block[j], block[j]), block[j])]

    @pl.when(is_inner)
    def _():
        for j in range(3):
            for layer in range(LAYERS):
                ref = last_piece(j, layer, centre)
                remote(ref, ref, send_sem.at[4, j], o_recv.at[j * LAYERS + layer], core(outer)).start()

    @pl.when(is_end)
    def _():
        for j in range(3):
            for layer in range(LAYERS):
                ref = last_piece(j, layer, 3 - near)
                remote(ref, ref, core_send.at[j], o_recv.at[j * LAYERS + layer], other_core).wait_recv()
                share(j, ref)

    wait_moments(ag_total - 2)
    wait_moments(ag_total - 1)

    def wait_send(ref, sem):
        remote(ref, ref, sem, sem, other_core).wait_send()

    for j in range(3):
        half = land[j].at[pl.ds(0, 4)]
        mine = land[j].at[pl.ds(0, LAYERS)]
        wait_send(land[j], peer_send.at[j])

        @pl.when(z != 0)
        def _():
            wait_send(half, sum_send.at[0, j])

        @pl.when(z != 3)
        def _():
            wait_send(half, sum_send.at[1, j])

        wait_send(mine, send_sem.at[0, j])
        wait_send(mine, send_sem.at[1, j])

        @pl.when(is_inner)
        def _():
            for sem in (2, 3, 4):
                wait_send(mine, send_sem.at[sem, j])

        wait_send(land[j], core_send.at[j])
        remote(land[j], land[j], core_send.at[j], core_recv.at[j], other_core).wait_recv()
        pltpu.make_async_copy(mine, peer[j].at[pl.ds(0, LAYERS)], local_sem.at[j]).wait()

    @pl.when(is_end)
    def _():
        for d in range(1, 8):
            norm_copy(d).wait_send()


def solution(mesh):
    def step(*arrays):
        terms, weights, m, v = (arrays[i : i + 3] for i in (0, 3, 6, 9))
        terms = [t.reshape(t.shape[1:]) for t in terms]
        shapes = [one.shape for one in m]
        count = sum(t.size for t in terms)
        rs_total = sum(LAYERS * 2 * s[1] // r for s, r in zip(shapes, RS_ROWS, strict=True))
        ag_total = sum(LAYERS * s[1] // r for s, r in zip(shapes, AG_ROWS, strict=True))
        units = [pltpu.VMEM((LAYERS * CHIPS, s[1], s[2]), jnp.bfloat16) for s in shapes]
        wide, tall = shapes[0], shapes[2]

        def pair(slots, rows, dtype):
            return [pltpu.VMEM((*slots, rows[0], wide[2]), dtype), pltpu.VMEM((*slots, rows[2], tall[2]), dtype)]

        dma = pltpu.SemaphoreType.DMA
        outs = pl.pallas_call(
            lambda *refs: kernel(count, *refs),
            out_shape=[jax.ShapeDtypeStruct(one.shape, jnp.bfloat16) for one in weights]
            + [jax.ShapeDtypeStruct(one.shape, jnp.float32) for one in (*m, *v)],
            in_specs=[pl.BlockSpec(memory_space=pl.ANY)] * 12,
            out_specs=[pl.BlockSpec(memory_space=pl.ANY)] * 9,
            scratch_shapes=units
            + units
            + pair((2, AHEAD + 1), RS_ROWS, jnp.bfloat16)
            + pair((READ + 1,), AG_ROWS, jnp.float32)
            + pair((READ + 1,), AG_ROWS, jnp.float32)
            + pair((READ + 1,), AG_ROWS, jnp.bfloat16)
            + pair((2,), AG_ROWS, jnp.float32)
            + pair((2,), AG_ROWS, jnp.float32)
            + [pltpu.VMEM((8, wide[2]), jnp.float32), pltpu.VMEM((8, tall[2]), jnp.float32)]
            + [pltpu.VMEM((8, 128), jnp.float32), pltpu.VMEM((4, 8, 128), jnp.float32)]
            + [
                dma((2, AHEAD + 1)),
                dma((3,)),
                dma((24,)),
                dma((2, 3)),
                dma((2, rs_total)),
                dma((7,)),
                dma((4,)),
                dma((3, READ + 1)),
                dma((2, 2)),
                dma((ag_total,)),
                dma((ag_total,)),
                dma((ag_total,)),
                dma((ag_total,)),
                dma((3 * LAYERS,)),
                dma((5, 3)),
                dma((3,)),
                dma((3,)),
                dma((3,)),
            ],
            name="clipped_step",
            compiler_params=pltpu.CompilerParams(collective_id=0, has_side_effects=True, vmem_limit_bytes=67043328),
        )(*terms, *weights, *m, *v)
        return tuple(outs)

    all_of, cut = P(None, None, None), P(None, "dp", None)
    return jax.shard_map(
        step,
        mesh=mesh,
        in_specs=(P(("rep", "dp"), None, None, None),) * 3 + (all_of,) * 3 + (cut,) * 6,
        out_specs=(P("rep", None, None),) * 3 + (P("rep", "dp", None),) * 6,
        check_vma=False,
    )
```

```python
import jax
import jax.numpy as jnp
from jax import lax
from jax.experimental import pallas as pl
from jax.experimental.pallas import tpu as pltpu
from jax.sharding import PartitionSpec as P


MESH = pl.DeviceIdType.MESH
CHIPS = 4
LAYERS = 2
RS_ROWS = (16, 16, 32)
AG_ROWS = (16, 16, 32)
LAG = 2
SINK_LAG = 12
NEW_LAG = 2
HANDED = 4
AHEAD = 3
READ = 2


def kernel(count, *refs):
    g, w, m, v = (refs[i : i + 3] for i in (0, 3, 6, 9))
    new_w, hand, new_m, new_v = (refs[i : i + 3] for i in (12, 15, 18, 21))
    refs = refs[3:]
    (land_0, land_1, land_2, peer_0, peer_1, peer_2, own_a, own_b, m_a, m_b, v_a, v_b, w_a, w_b, mo_a, mo_b, vo_a, vo_b) = refs[21:39]
    (squares_a, squares_b, part, norms) = refs[39:43]
    (own_sem, peer_send, peer_recv, sum_send, sum_recv, norm_send, norm_recv, tile_sem, out_sem, g_recv, e_recv, i_recv, f_recv) = refs[43:56]
    (send_sem, core_send, core_recv, local_sem) = refs[56:]
    land, peer = (land_0, land_1, land_2), (peer_0, peer_1, peer_2)
    own, m_in, v_in, w_in = (own_a, own_a, own_b), (m_a, m_a, m_b), (v_a, v_a, v_b), (w_a, w_a, w_b)
    m_out, v_out, squares = (mo_a, mo_a, mo_b), (vo_a, vo_a, vo_b), (squares_a, squares_a, squares_b)
    block = [ref.shape[1] for ref in land]
    f32 = jnp.float32

    me = lax.axis_index("dp")
    z, c = lax.div(me, 2), lax.rem(me, 2)
    is_end = (z == 0) | (z == 3)
    is_inner = jnp.logical_not(is_end)
    centre = jnp.where(z == 0, 1, jnp.where(z == 3, 2, 3 - z))
    outer = jnp.where(z <= 1, 0, 3)

    def core(chip):
        return {"dp": chip * 2 + c}

    other_core = {"dp": z * 2 + 1 - c}

    def remote(src, dst, send, recv, device):
        return pltpu.make_async_remote_copy(src_ref=src, dst_ref=dst, send_sem=send, recv_sem=recv, device_id=device, device_id_type=MESH)

    barrier = pltpu.get_barrier_semaphore()
    for d in range(1, 8):
        pl.semaphore_signal(barrier, inc=1, device_id={"dp": lax.rem(me + d, 8)}, device_id_type=MESH)
    pl.semaphore_wait(barrier, 7)

    def unit_of(layer, chip):
        return layer * CHIPS + chip

    def push_terms(j, layer, chip):
        u = unit_of(layer, chip)
        rows = pl.ds(pl.multiple_of((chip * 2 + 1 - c) * block[j], block[j]), block[j])
        return remote(g[j].at[layer, rows], peer[j].at[u], peer_send.at[j], peer_recv.at[j * 8 + u], other_core)

    for j in range(3):
        for layer in range(LAYERS):
            for o in range(2):
                push_terms(j, layer, o).start()
                push_terms(j, layer, 2 + o).start()

    rs_n = [block[j] // RS_ROWS[j] for j in range(3)]
    rs_k = [LAYERS * 2 * n for n in rs_n]
    rs_total = sum(rs_k)
    ag_n = [block[j] // AG_ROWS[j] for j in range(3)]
    ag_k = [LAYERS * n for n in ag_n]
    ag_total = sum(ag_k)

    def each(counts, k, body):
        first = 0
        for j in range(3):
            last = first + counts[j]

            @pl.when((k >= first) & (k < last))
            def _(j=j, first=first):
                body(j, k - first)

            first = last

    def rs_piece(flow, j, k):
        unit, s = lax.div(k, rs_n[j]), lax.rem(k, rs_n[j])
        layer, chip = lax.div(unit, 2), lax.rem(unit, 2) + 2 * flow
        return layer, chip, s

    def rows_of(j, device, s, n):
        return pl.ds(pl.multiple_of(device * block[j] + s * n, n), n)

    def load_terms(flow, j, k, slot):
        layer, chip, s = rs_piece(flow, j, k)
        rows = rows_of(j, chip * 2 + c, s, RS_ROWS[j])
        return pltpu.make_async_copy(g[j].at[layer, rows], own[j].at[flow, slot], own_sem.at[flow, slot])

    for ref in (squares_a, squares_b):
        ref[...] = jnp.zeros_like(ref)

    def sum_step(flow, i):
        source, sink = (3, 0) if flow == 0 else (0, 3)
        hops = 3 - z if flow == 0 else z
        lag = jnp.where(hops == 3, SINK_LAG, jnp.where(hops == 2, LAG, 0))
        to = z - 1 if flow == 0 else z + 1
        k = i - lag
        each(rs_k, k + AHEAD, lambda j, q: load_terms(flow, j, q, lax.rem(k + AHEAD, AHEAD + 1)).start())

        def body(j, q):
            layer, chip, s = rs_piece(flow, j, q)
            u, n, slot = unit_of(layer, chip), RS_ROWS[j], lax.rem(k, AHEAD + 1)
            rows = pl.ds(pl.multiple_of(s * n, n), n)
            here = land[j].at[u, rows]
            load_terms(flow, j, q, slot).wait()

            @pl.when(s == 0)
            def _():
                remote(peer[j].at[u], peer[j].at[u], peer_send.at[j], peer_recv.at[j * 8 + u], other_core).wait_recv()

            copy = remote(here, here, sum_send.at[flow, j], sum_recv.at[flow, k], core(jnp.clip(to, 0, 3)))

            @pl.when(z != source)
            def _():
                copy.wait_recv()

            def add(fed, last):
                for r in range(0, n, 16):
                    at = pl.ds(pl.multiple_of(s * n + r, 16), 16)
                    total = own[j][flow, slot, pl.ds(r, 16)].astype(f32) + peer[j][u, at].astype(f32)
                    if fed:
                        total = land[j][u, at].astype(f32) + total
                    total = total.astype(jnp.bfloat16)
                    land[j][u, at] = total
                    if last:
                        total = total.astype(f32)
                        total = total * total
                        squares[j][...] += total[:8] + total[8:]

            @pl.when(z == source)
            def _():
                add(False, False)

            @pl.when((z != source) & (z != sink))
            def _():
                add(True, False)

            @pl.when(z == sink)
            def _():
                add(True, True)

            @pl.when(z != sink)
            def _():
                copy.start()

        each(rs_k, k, body)

    def both(i, carry):
        sum_step(0, i - AHEAD)
        sum_step(1, i - AHEAD)
        return carry

    def ag_piece(j, k):
        layer, s = lax.div(k, ag_n[j]), lax.rem(k, ag_n[j])
        return layer, s

    def tiles(j, k, slot):
        layer, s = ag_piece(j, k)
        n = AG_ROWS[j]
        rows = pl.ds(pl.multiple_of(s * n, n), n)
        return (
            pltpu.make_async_copy(m[j].at[layer, rows], m_in[j].at[slot], tile_sem.at[0, slot]),
            pltpu.make_async_copy(v[j].at[layer, rows], v_in[j].at[slot], tile_sem.at[1, slot]),
            pltpu.make_async_copy(w[j].at[layer, rows_of(j, me, s, n)], w_in[j].at[slot], tile_sem.at[2, slot]),
        )

    def start_tiles(k):
        def body(j, q):
            for copy in tiles(j, q, lax.rem(k, READ + 1)):
                copy.start()

        each(ag_k, k, body)

    for k in range(READ):
        for copy in tiles(0, k, k):
            copy.start()

    lax.fori_loop(0, rs_total + AHEAD + SINK_LAG, both, 0)

    def hand_on(k):
        def body(j, q):
            layer, s = ag_piece(j, q)
            n = AG_ROWS[j]
            u, rows = unit_of(layer, centre), pl.ds(pl.multiple_of(s * n, n), n)
            remote(land[j].at[u, rows], peer[j].at[u, rows], send_sem.at[0, j], g_recv.at[k], core(centre)).start()

        each(ag_k, k, body)

    @pl.when(is_end)
    def _():
        for k in range(HANDED):
            hand_on(jnp.int32(k))

    place = jnp.where(z == 0, c, 2 + c)

    def norm_copy(d):
        return remote(part, norms.at[place], norm_send.at[d - 1], norm_recv.at[place], {"dp": lax.rem(me + d, 8)})

    @pl.when(is_end)
    def _():
        total = jnp.sum(squares_a[...]) + jnp.sum(squares_b[...])
        part[...] = jnp.full(part.shape, total, f32)
        norms[place] = jnp.full(part.shape, total, f32)
        for d in range(1, 8):
            norm_copy(d).start()

    for p in range(4):

        @pl.when(is_inner | (place != p))
        def _():
            remote(part, norms.at[p], norm_send.at[0], norm_recv.at[p], other_core).wait_recv()

    total = norms[0] + norms[1] + norms[2] + norms[3]
    factor = jnp.minimum(1.0, 0.5 * lax.rsqrt(total / count + 1e-30))[:1, :1]

    def new_piece(j, k, chip):
        layer, s = ag_piece(j, k)
        return new_w[j].at[layer, rows_of(j, chip * 2 + c, s, AG_ROWS[j])]


    def moments_out(j, k, slot):
        layer, s = ag_piece(j, k)
        n = AG_ROWS[j]
        rows = pl.ds(pl.multiple_of(s * n, n), n)
        return (
            pltpu.make_async_copy(m_out[j].at[slot], new_m[j].at[layer, rows], out_sem.at[0, slot]),
            pltpu.make_async_copy(v_out[j].at[slot], new_v[j].at[layer, rows], out_sem.at[1, slot]),
        )

    def wait_moments(k):
        def body(j, q):
            for copy in moments_out(j, q, lax.rem(k, 2)):
                copy.wait()

        each(ag_k, k, body)

    def own_step(k):
        def body(j, q):
            start_tiles(k + READ)
            wait_moments(k - 2)
            layer, s = ag_piece(j, q)
            n, slot, out = AG_ROWS[j], lax.rem(k, READ + 1), lax.rem(k, 2)
            rows = pl.ds(pl.multiple_of(s * n, n), n)
            u_own, u_new = unit_of(layer, z), unit_of(layer, lax.bitwise_xor(z, 1))

            for copy in tiles(j, q, slot):
                copy.wait()

            @pl.when(is_inner)
            def _():
                remote(land[j].at[u_own, rows], peer[j].at[u_own, rows], send_sem.at[0, j], g_recv.at[k], core(centre)).wait_recv()

            def update(sums):
                for r in range(0, n, 16):
                    at, tile = pl.ds(pl.multiple_of(s * n + r, 16), 16), pl.ds(r, 16)
                    clipped = sums[j][u_own, at].astype(f32) * factor
                    one_m = 0.9 * m_in[j][slot, tile] + 0.1 * clipped
                    one_v = 0.95 * v_in[j][slot, tile] + 0.05 * clipped * clipped
                    one_w = w_in[j][slot, tile].astype(f32)
                    step = one_m * lax.rsqrt(one_v + 1e-8) + 0.1 * one_w
                    m_out[j][out, tile] = one_m
                    v_out[j][out, tile] = one_v
                    peer[j][u_new, at] = (one_w - 0.02 * step).astype(jnp.bfloat16)

            @pl.when(is_end)
            def _():
                update(land)

            @pl.when(is_inner)
            def _():
                update(peer)

            for copy in moments_out(j, q, out):
                copy.start()
            ready, there = peer[j].at[u_new, rows], new_piece(j, q, z)

            @pl.when(is_end)
            def _():
                remote(ready, there, send_sem.at[1, j], e_recv.at[k], core(centre)).start()
                hand_on(k + HANDED)

            @pl.when(is_inner)
            def _():
                remote(ready, there, send_sem.at[0, j], i_recv.at[k], core(outer)).start()
                remote(ready, hand[j].at[layer, rows], send_sem.at[1, j], i_recv.at[k], core(centre)).start()

            remote(ready, there, core_send.at[j], core_recv.at[j], other_core).start()
            pltpu.make_async_copy(ready, there, local_sem.at[j]).start()

        each(ag_k, k, body)

    def arrived(k, chip, recv, forward=None, handed=False):
        def body(j, q):
            ref = there = new_piece(j, q, chip)
            if handed:
                layer, s = ag_piece(j, q)
                ref = hand[j].at[layer, pl.ds(pl.multiple_of(s * AG_ROWS[j], AG_ROWS[j]), AG_ROWS[j])]
            remote(ref, ref, core_send.at[j], recv.at[k], other_core).wait_recv()
            if forward is not None:
                sem, to = forward
                remote(ref, ref, send_sem.at[sem, j], f_recv.at[k], core(to)).start()
            remote(ref, there, core_send.at[j], core_recv.at[j], other_core).start()

        each(ag_k, k, body)

    near, far = jnp.where(z <= 1, 1, 2), 3 - outer

    def new_step(i, carry):
        @pl.when(is_end)
        def _():
            own_step(i)
            arrived(i - NEW_LAG, near, i_recv)
            arrived(i - 3 * NEW_LAG, far, f_recv)

        @pl.when(is_inner)
        def _():
            own_step(i)
            arrived(i - 2 * NEW_LAG, far, f_recv, (3, outer))
            arrived(i - NEW_LAG, outer, e_recv, (2, centre))
            arrived(i - NEW_LAG, centre, i_recv, handed=True)

        return carry

    lax.fori_loop(0, ag_total + 3 * NEW_LAG, new_step, 0)

    wait_moments(ag_total - 2)
    wait_moments(ag_total - 1)

    def wait_send(ref, sem):
        remote(ref, ref, sem, sem, other_core).wait_send()

    for j in range(3):
        half = land[j].at[pl.ds(0, 4)]
        mine = land[j].at[pl.ds(0, LAYERS)]
        wait_send(land[j], peer_send.at[j])

        @pl.when(z != 0)
        def _():
            wait_send(half, sum_send.at[0, j])

        @pl.when(z != 3)
        def _():
            wait_send(half, sum_send.at[1, j])

        wait_send(mine, send_sem.at[0, j])
        wait_send(mine, send_sem.at[1, j])

        @pl.when(is_inner)
        def _():
            for sem in (2, 3):
                wait_send(mine, send_sem.at[sem, j])

        def wait_core(ref):
            wait_send(ref, core_send.at[j])
            remote(ref, ref, core_send.at[j], core_recv.at[j], other_core).wait_recv()

        @pl.when(is_end)
        def _():
            wait_core(land[j].at[pl.ds(0, 3 * LAYERS)])

        @pl.when(is_inner)
        def _():
            wait_core(land[j])

        pltpu.make_async_copy(mine, peer[j].at[pl.ds(0, LAYERS)], local_sem.at[j]).wait()

    @pl.when(is_end)
    def _():
        for d in range(1, 8):
            norm_copy(d).wait_send()


def settle(parts, *refs):
    w, hand, rest, results = refs[:3], refs[3:6], refs[6:12], refs[12:21]
    slots, (in_sem, out_sem) = refs[21:25], refs[25:]
    me = lax.axis_index("dp")
    z, c = lax.div(me, 2), lax.rem(me, 2)
    is_inner = (z == 1) | (z == 2)
    items, used = [], [0] * 4

    def item(pool, src, dst, other=None, chosen=None):
        items.append((pool, used[pool] % slots[pool].shape[0], src, dst, other, chosen))
        used[pool] += 1

    for j in range(3):
        rows = w[j].shape[1] // (2 * CHIPS)
        for layer in range(LAYERS):
            for d in range(2 * CHIPS):
                at = (layer, pl.ds(d * rows, rows))
                item(j // 2, w[j].at[at], results[j].at[at], hand[j].at[layer], is_inner & (d == (3 - z) * 2 + c))
    for i in range(6):
        for layer in range(LAYERS):
            item(2 + i % 3 // 2, rest[i].at[layer], results[3 + i].at[layer])

    def get(t, src):
        pool, slot = items[t][:2]
        return pltpu.make_async_copy(src, slots[pool].at[slot], in_sem.at[pool, slot])

    def put(t):
        pool, slot, _, dst = items[t][:4]
        return pltpu.make_async_copy(slots[pool].at[slot], dst, out_sem.at[pool, slot])

    busy = {}
    for t in range(len(items) + parts):
        if t < len(items):
            pool, slot, src, _, other, chosen = items[t]
            if (pool, slot) in busy:
                put(busy.pop((pool, slot))).wait()
            if other is None:
                get(t, src).start()
            else:

                @pl.when(chosen)
                def _():
                    get(t, other).start()

                @pl.when(jnp.logical_not(chosen))
                def _():
                    get(t, src).start()

        if t >= parts:
            done = t - parts
            get(done, items[done][2]).wait()
            put(done).start()
            busy[items[done][:2]] = done
    for t in busy.values():
        put(t).wait()


def place(n, *refs):
    mine, others, results, buffers = (refs[i * n : (i + 1) * n] for i in (1, 2, 3, 4))
    in_sem, out_sem = refs[5 * n :]
    me = lax.axis_index("dp")
    z, c = lax.div(me, 2), lax.rem(me, 2)

    @pl.when((z == 0) | (z == 3))
    def _():
        chip = jnp.where(z == 0, 2, 1)
        gets, puts = [], []
        for j in range(n):
            rows = mine[j].shape[1]
            for b, (src, core) in enumerate(((mine[j], c), (others[j], 1 - c))):
                for layer in range(LAYERS):
                    at = pl.ds(pl.multiple_of((chip * 2 + core) * rows, rows), rows)
                    gets.append(pltpu.make_async_copy(src.at[layer], buffers[j].at[b, layer], in_sem.at[j, b, layer]))
                    puts.append(pltpu.make_async_copy(buffers[j].at[b, layer], results[j].at[layer, at], out_sem.at[j, b, layer]))
        for copy in gets:
            copy.start()
        for get, put in zip(gets, puts, strict=True):
            get.wait()
            put.start()
        for copy in puts:
            copy.wait()


def solution(mesh):
    def step(*arrays):
        terms, weights, m, v = (arrays[i : i + 3] for i in (0, 3, 6, 9))
        terms = [t.reshape(t.shape[1:]) for t in terms]
        shapes = [one.shape for one in m]
        count = sum(t.size for t in terms)
        rs_total = sum(LAYERS * 2 * s[1] // r for s, r in zip(shapes, RS_ROWS, strict=True))
        ag_total = sum(LAYERS * s[1] // r for s, r in zip(shapes, AG_ROWS, strict=True))
        units = [pltpu.VMEM((LAYERS * CHIPS, s[1], s[2]), jnp.bfloat16) for s in shapes]
        wide, tall = shapes[0], shapes[2]

        def pair(slots, rows, dtype):
            return [pltpu.VMEM((*slots, rows[0], wide[2]), dtype), pltpu.VMEM((*slots, rows[2], tall[2]), dtype)]

        dma = pltpu.SemaphoreType.DMA
        outs = pl.pallas_call(
            lambda *refs: kernel(count, *refs),
            out_shape=[jax.ShapeDtypeStruct(one.shape, jnp.bfloat16) for one in weights]
            + [jax.ShapeDtypeStruct(one.shape, jnp.bfloat16) for one in m]
            + [jax.ShapeDtypeStruct(one.shape, jnp.float32) for one in (*m, *v)],
            in_specs=[pl.BlockSpec(memory_space=pl.ANY)] * 12,
            out_specs=[pl.BlockSpec(memory_space=pl.ANY)] * 12,
            scratch_shapes=units
            + units
            + pair((2, AHEAD + 1), RS_ROWS, jnp.bfloat16)
            + pair((READ + 1,), AG_ROWS, jnp.float32)
            + pair((READ + 1,), AG_ROWS, jnp.float32)
            + pair((READ + 1,), AG_ROWS, jnp.bfloat16)
            + pair((2,), AG_ROWS, jnp.float32)
            + pair((2,), AG_ROWS, jnp.float32)
            + [pltpu.VMEM((8, wide[2]), jnp.float32), pltpu.VMEM((8, tall[2]), jnp.float32)]
            + [pltpu.VMEM((8, 128), jnp.float32), pltpu.VMEM((4, 8, 128), jnp.float32)]
            + [
                dma((2, AHEAD + 1)),
                dma((3,)),
                dma((24,)),
                dma((2, 3)),
                dma((2, rs_total)),
                dma((7,)),
                dma((4,)),
                dma((3, READ + 1)),
                dma((2, 2)),
                dma((ag_total,)),
                dma((ag_total,)),
                dma((ag_total,)),
                dma((ag_total,)),
                dma((4, 3)),
                dma((3,)),
                dma((3,)),
                dma((3,)),
            ],
            name="clipped_step",
            compiler_params=pltpu.CompilerParams(collective_id=0, has_side_effects=True, vmem_limit_bytes=67043328),
        )(*terms, *weights, *m, *v)
        whole, hand, rest = outs[:3], outs[3:6], outs[6:]
        came = []
        for one in hand:
            came.append(lax.ppermute(one, "dp", [(2, 0), (3, 1), (4, 6), (5, 7)]))
        any_space = pl.BlockSpec(memory_space=pl.ANY)
        results = pl.pallas_call(
            lambda *refs: settle(4, *refs),
            out_shape=[jax.ShapeDtypeStruct(one.shape, one.dtype) for one in (*whole, *rest)],
            in_specs=[any_space] * 12,
            out_specs=[any_space] * 9,
            scratch_shapes=[
                pltpu.VMEM((8, *wide[1:]), jnp.bfloat16),
                pltpu.VMEM((8, *tall[1:]), jnp.bfloat16),
                pltpu.VMEM((6, *wide[1:]), jnp.float32),
                pltpu.VMEM((4, *tall[1:]), jnp.float32),
                dma((4, 8)),
                dma((4, 8)),
            ],
            name="settle",
            cost_estimate=pl.CostEstimate(flops=10**9, bytes_accessed=141 * 10**6, transcendentals=0),
            compiler_params=pltpu.CompilerParams(vmem_limit_bytes=62 * 2**20),
        )(*whole, *hand, *rest)
        others = []
        for j in range(3):
            came[j], _ = lax.optimization_barrier((came[j], results[3]))
            others.append(lax.ppermute(came[j], "dp", [(0, 1), (1, 0), (6, 7), (7, 6)]))

        def put(which):
            n = len(which)
            return pl.pallas_call(
                lambda *refs: place(n, *refs),
                out_shape=[jax.ShapeDtypeStruct(results[j].shape, results[j].dtype) for j in which],
                in_specs=[any_space] * (3 * n),
                out_specs=[any_space] * n,
                scratch_shapes=[pltpu.VMEM((2, *hand[j].shape), jnp.bfloat16) for j in which] + [dma((n, 2, LAYERS)), dma((n, 2, LAYERS))],
                input_output_aliases={i: i for i in range(n)},
                name="place",
                cost_estimate=pl.CostEstimate(flops=10**7, bytes_accessed=n * 16 * 10**6, transcendentals=0),
            )(*(results[j] for j in which), *(came[j] for j in which), *(others[j] for j in which))

        early = put((0, 1))
        late = put((2,))
        return (*early, *late, *results[3:])

    all_of, cut = P(None, None, None), P(None, "dp", None)
    return jax.shard_map(
        step,
        mesh=mesh,
        in_specs=(P(("rep", "dp"), None, None, None),) * 3 + (all_of,) * 3 + (cut,) * 6,
        out_specs=(P("rep", None, None),) * 3 + (P("rep", "dp", None),) * 6,
        check_vma=False,
    )
```

```python
import jax
import jax.numpy as jnp
from jax import lax
from jax.experimental import pallas as pl
from jax.experimental.pallas import tpu as pltpu
from jax.sharding import PartitionSpec as P


MESH = pl.DeviceIdType.MESH
CHIPS = 4
LAYERS = 2
RS_ROWS = (16, 16, 32)
AG_ROWS = (16, 16, 32)
LAG = 2
SINK_LAG = 12
NEW_LAG = 2
END_LAG = 20
HANDED = 3
AHEAD = 3
READ = 2


def kernel(count, *refs):
    g, w, m, v = (refs[i : i + 3] for i in (0, 3, 6, 9))
    new_w, new_m, new_v = (refs[i : i + 3] for i in (12, 17, 20))
    hand = (None, *refs[15:17])
    refs = refs[2:]
    (land_0, land_1, land_2, peer_0, peer_1, peer_2, own_a, own_b, m_a, m_b, v_a, v_b, w_a, w_b, mo_a, mo_b, vo_a, vo_b) = refs[21:39]
    (squares_a, squares_b, part, norms) = refs[39:43]
    (own_sem, peer_send, peer_recv, sum_send, sum_recv, norm_send, norm_recv, tile_sem, out_sem, g_recv, e_recv, i_recv, f_recv, o_recv) = refs[43:57]
    (send_sem, core_send, core_recv, local_sem) = refs[57:]
    land, peer = (land_0, land_1, land_2), (peer_0, peer_1, peer_2)
    own, m_in, v_in, w_in = (own_a, own_a, own_b), (m_a, m_a, m_b), (v_a, v_a, v_b), (w_a, w_a, w_b)
    m_out, v_out, squares = (mo_a, mo_a, mo_b), (vo_a, vo_a, vo_b), (squares_a, squares_a, squares_b)
    block = [ref.shape[1] for ref in land]
    f32 = jnp.float32

    me = lax.axis_index("dp")
    z, c = lax.div(me, 2), lax.rem(me, 2)
    is_end = (z == 0) | (z == 3)
    is_inner = jnp.logical_not(is_end)
    centre = jnp.where(z == 0, 1, jnp.where(z == 3, 2, 3 - z))
    outer = jnp.where(z <= 1, 0, 3)

    def core(chip):
        return {"dp": chip * 2 + c}

    other_core = {"dp": z * 2 + 1 - c}

    def remote(src, dst, send, recv, device):
        return pltpu.make_async_remote_copy(src_ref=src, dst_ref=dst, send_sem=send, recv_sem=recv, device_id=device, device_id_type=MESH)

    barrier = pltpu.get_barrier_semaphore()
    for d in range(1, 8):
        pl.semaphore_signal(barrier, inc=1, device_id={"dp": lax.rem(me + d, 8)}, device_id_type=MESH)
    pl.semaphore_wait(barrier, 7)

    def unit_of(layer, chip):
        return layer * CHIPS + chip

    def push_terms(j, layer, chip):
        u = unit_of(layer, chip)
        rows = pl.ds(pl.multiple_of((chip * 2 + 1 - c) * block[j], block[j]), block[j])
        return remote(g[j].at[layer, rows], peer[j].at[u], peer_send.at[j], peer_recv.at[j * 8 + u], other_core)

    @pl.when(z <= 1)
    def _():
        push_terms(0, 0, 2).start()
        push_terms(0, 0, 0).start()

    @pl.when(z > 1)
    def _():
        push_terms(0, 0, 0).start()
        push_terms(0, 0, 2).start()

    push_terms(0, 0, 1).start()
    push_terms(0, 0, 3).start()

    rs_n = [block[j] // RS_ROWS[j] for j in range(3)]
    rs_k = [LAYERS * 2 * n for n in rs_n]
    rs_total = sum(rs_k)
    ag_n = [block[j] // AG_ROWS[j] for j in range(3)]
    ag_k = [LAYERS * n for n in ag_n]
    ag_total = sum(ag_k)

    def each(counts, k, body):
        first = 0
        for j in range(3):
            last = first + counts[j]

            @pl.when((k >= first) & (k < last))
            def _(j=j, first=first):
                body(j, k - first)

            first = last

    def rs_piece(flow, j, k):
        unit, s = lax.div(k, rs_n[j]), lax.rem(k, rs_n[j])
        layer, chip = lax.div(unit, 2), lax.rem(unit, 2) + 2 * flow
        return layer, chip, s

    def rows_of(j, device, s, n):
        return pl.ds(pl.multiple_of(device * block[j] + s * n, n), n)

    def load_terms(flow, j, k, slot):
        layer, chip, s = rs_piece(flow, j, k)
        rows = rows_of(j, chip * 2 + c, s, RS_ROWS[j])
        return pltpu.make_async_copy(g[j].at[layer, rows], own[j].at[flow, slot], own_sem.at[flow, slot])

    def push_unit(flow, x):
        each((2 * LAYERS,) * 3, x, lambda j, y: push_terms(j, lax.div(y, 2), lax.rem(y, 2) + 2 * flow).start())

    for ref in (squares_a, squares_b):
        ref[...] = jnp.zeros_like(ref)

    def sum_step(flow, i):
        source, sink = (3, 0) if flow == 0 else (0, 3)
        hops = 3 - z if flow == 0 else z
        lag = jnp.where(hops == 3, SINK_LAG, jnp.where(hops == 2, LAG, 0))
        to = z - 1 if flow == 0 else z + 1
        k = i - lag
        each(rs_k, k + AHEAD, lambda j, q: load_terms(flow, j, q, lax.rem(k + AHEAD, AHEAD + 1)).start())

        def body(j, q):
            layer, chip, s = rs_piece(flow, j, q)
            u, n, slot = unit_of(layer, chip), RS_ROWS[j], lax.rem(k, AHEAD + 1)
            rows = pl.ds(pl.multiple_of(s * n, n), n)
            here = land[j].at[u, rows]
            load_terms(flow, j, q, slot).wait()

            @pl.when(s == 0)
            def _():
                push_unit(flow, j * 2 * LAYERS + lax.div(q, rs_n[j]) + 2)
                remote(peer[j].at[u], peer[j].at[u], peer_send.at[j], peer_recv.at[j * 8 + u], other_core).wait_recv()

            copy = remote(here, here, sum_send.at[flow, j], sum_recv.at[flow, k], core(jnp.clip(to, 0, 3)))

            @pl.when(z != source)
            def _():
                copy.wait_recv()

            def add(fed, last):
                for r in range(0, n, 16):
                    at = pl.ds(pl.multiple_of(s * n + r, 16), 16)
                    total = own[j][flow, slot, pl.ds(r, 16)].astype(f32) + peer[j][u, at].astype(f32)
                    if fed:
                        total = land[j][u, at].astype(f32) + total
                    total = total.astype(jnp.bfloat16)
                    land[j][u, at] = total
                    if last:
                        total = total.astype(f32)
                        total = total * total
                        squares[j][...] += total[:8] + total[8:]

            @pl.when(z == source)
            def _():
                add(False, False)

            @pl.when((z != source) & (z != sink))
            def _():
                add(True, False)

            @pl.when(z == sink)
            def _():
                add(True, True)

            @pl.when(z != sink)
            def _():
                copy.start()

        each(rs_k, k, body)

    def both(i, carry):
        sum_step(0, i - AHEAD)
        sum_step(1, i - AHEAD)
        return carry

    def ag_piece(j, k):
        layer, s = lax.div(k, ag_n[j]), lax.rem(k, ag_n[j])
        return layer, s

    def tiles(j, k, slot):
        layer, s = ag_piece(j, k)
        n = AG_ROWS[j]
        rows = pl.ds(pl.multiple_of(s * n, n), n)
        return (
            pltpu.make_async_copy(m[j].at[layer, rows], m_in[j].at[slot], tile_sem.at[0, slot]),
            pltpu.make_async_copy(v[j].at[layer, rows], v_in[j].at[slot], tile_sem.at[1, slot]),
            pltpu.make_async_copy(w[j].at[layer, rows_of(j, me, s, n)], w_in[j].at[slot], tile_sem.at[2, slot]),
        )

    def start_tiles(k):
        def body(j, q):
            for copy in tiles(j, q, lax.rem(k, READ + 1)):
                copy.start()

        each(ag_k, k, body)

    for k in range(READ):
        for copy in tiles(0, k, k):
            copy.start()

    lax.fori_loop(0, rs_total + AHEAD + SINK_LAG, both, 0)

    def hand_on(k):
        def body(j, q):
            layer, s = ag_piece(j, q)
            n = AG_ROWS[j]
            u, rows = unit_of(layer, centre), pl.ds(pl.multiple_of(s * n, n), n)
            remote(land[j].at[u, rows], peer[j].at[u, rows], send_sem.at[0, j], g_recv.at[k], core(centre)).start()

        each(ag_k, k, body)

    place = jnp.where(z == 0, c, 2 + c)

    def norm_copy(d):
        return remote(part, norms.at[place], norm_send.at[d - 1], norm_recv.at[place], {"dp": lax.rem(me + d, 8)})

    @pl.when(is_end)
    def _():
        total = jnp.sum(squares_a[...]) + jnp.sum(squares_b[...])
        part[...] = jnp.full(part.shape, total, f32)
        norms[place] = jnp.full(part.shape, total, f32)
        for d in range(1, 8):
            norm_copy(d).start()
        for k in range(HANDED):
            hand_on(jnp.int32(k))

    for p in range(4):

        @pl.when(is_inner | (place != p))
        def _():
            remote(part, norms.at[p], norm_send.at[0], norm_recv.at[p], other_core).wait_recv()

    total = norms[0] + norms[1] + norms[2] + norms[3]
    factor = jnp.minimum(1.0, 0.5 * lax.rsqrt(total / count + 1e-30))[:1, :1]

    def new_piece(j, k, chip):
        layer, s = ag_piece(j, k)
        return new_w[j].at[layer, rows_of(j, chip * 2 + c, s, AG_ROWS[j])]


    def moments_out(j, k, slot):
        layer, s = ag_piece(j, k)
        n = AG_ROWS[j]
        rows = pl.ds(pl.multiple_of(s * n, n), n)
        return (
            pltpu.make_async_copy(m_out[j].at[slot], new_m[j].at[layer, rows], out_sem.at[0, slot]),
            pltpu.make_async_copy(v_out[j].at[slot], new_v[j].at[layer, rows], out_sem.at[1, slot]),
        )

    def wait_moments(k):
        def body(j, q):
            for copy in moments_out(j, q, lax.rem(k, 2)):
                copy.wait()

        each(ag_k, k, body)

    def own_step(k):
        def body(j, q):
            start_tiles(k + READ)
            wait_moments(k - 2)
            layer, s = ag_piece(j, q)
            n, slot, out = AG_ROWS[j], lax.rem(k, READ + 1), lax.rem(k, 2)
            rows = pl.ds(pl.multiple_of(s * n, n), n)
            u_own, u_new = unit_of(layer, z), unit_of(layer, lax.bitwise_xor(z, 1))

            for copy in tiles(j, q, slot):
                copy.wait()

            @pl.when(is_inner)
            def _():
                remote(land[j].at[u_own, rows], peer[j].at[u_own, rows], send_sem.at[0, j], g_recv.at[k], core(centre)).wait_recv()

            def update(sums):
                for r in range(0, n, 16):
                    at, tile = pl.ds(pl.multiple_of(s * n + r, 16), 16), pl.ds(r, 16)
                    clipped = sums[j][u_own, at].astype(f32) * factor
                    one_m = 0.9 * m_in[j][slot, tile] + 0.1 * clipped
                    one_v = 0.95 * v_in[j][slot, tile] + 0.05 * clipped * clipped
                    one_w = w_in[j][slot, tile].astype(f32)
                    step = one_m * lax.rsqrt(one_v + 1e-8) + 0.1 * one_w
                    m_out[j][out, tile] = one_m
                    v_out[j][out, tile] = one_v
                    peer[j][u_new, at] = (one_w - 0.02 * step).astype(jnp.bfloat16)

            @pl.when(is_end)
            def _():
                update(land)

            @pl.when(is_inner)
            def _():
                update(peer)

            for copy in moments_out(j, q, out):
                copy.start()
            ready, there = peer[j].at[u_new, rows], new_piece(j, q, z)

            @pl.when(is_end)
            def _():
                remote(ready, there, send_sem.at[1, j], e_recv.at[k], core(centre)).start()
                hand_on(k + HANDED)

            @pl.when(is_inner)
            def _():
                remote(ready, there, send_sem.at[0, j], i_recv.at[k], core(outer)).start()
                remote(ready, hand[j].at[layer, rows] if j else there, send_sem.at[1, j], i_recv.at[k], core(centre)).start()

            remote(ready, there, core_send.at[j], core_recv.at[j], other_core).start()
            pltpu.make_async_copy(ready, there, local_sem.at[j]).start()

        each(ag_k, k, body)

    def arrived(k, chip, recv, forward=None, handed=False, which=range(3)):
        def body(j, q):
            if j not in which:
                return
            ref = there = new_piece(j, q, chip)
            if handed and j:
                layer, s = ag_piece(j, q)
                ref = hand[j].at[layer, pl.ds(pl.multiple_of(s * AG_ROWS[j], AG_ROWS[j]), AG_ROWS[j])]
            remote(ref, ref, core_send.at[j], recv.at[k], other_core).wait_recv()
            if forward is not None and not (handed and j):
                sem, there_recv, to = forward
                remote(ref, ref, send_sem.at[sem, j], there_recv.at[k], core(to)).start()
            remote(ref, there, core_send.at[j], core_recv.at[j], other_core).start()

        each(ag_k, k, body)

    near, far = jnp.where(z <= 1, 1, 2), 3 - outer

    def new_step(i, carry):
        @pl.when(is_end)
        def _():
            own_step(i)
            arrived(i - END_LAG, near, i_recv)
            arrived(i - END_LAG, far, f_recv)
            arrived(i - END_LAG, 3 - near, o_recv, which=(0,))

        @pl.when(is_inner)
        def _():
            own_step(i)
            arrived(i - 2 * NEW_LAG, far, f_recv, (3, f_recv, outer))
            arrived(i - NEW_LAG, outer, e_recv, (2, f_recv, centre))
            arrived(i - NEW_LAG, centre, i_recv, (4, o_recv, outer), handed=True)

        return carry

    lax.fori_loop(0, ag_total + END_LAG, new_step, 0)

    wait_moments(ag_total - 2)
    wait_moments(ag_total - 1)

    def wait_send(ref, sem):
        remote(ref, ref, sem, sem, other_core).wait_send()

    for j in range(3):
        half = land[j].at[pl.ds(0, 4)]
        mine = land[j].at[pl.ds(0, LAYERS)]
        wait_send(land[j], peer_send.at[j])

        @pl.when(z != 0)
        def _():
            wait_send(half, sum_send.at[0, j])

        @pl.when(z != 3)
        def _():
            wait_send(half, sum_send.at[1, j])

        wait_send(mine, send_sem.at[0, j])
        wait_send(mine, send_sem.at[1, j])

        @pl.when(is_inner)
        def _():
            for sem in (2, 3, 4) if j == 0 else (2, 3):
                wait_send(mine, send_sem.at[sem, j])

        def wait_core(ref):
            wait_send(ref, core_send.at[j])
            remote(ref, ref, core_send.at[j], core_recv.at[j], other_core).wait_recv()

        @pl.when(is_end)
        def _():
            wait_core(land[j].at[pl.ds(0, 3 * LAYERS)] if j else land[j])

        @pl.when(is_inner)
        def _():
            wait_core(land[j])

        pltpu.make_async_copy(mine, peer[j].at[pl.ds(0, LAYERS)], local_sem.at[j]).wait()

    @pl.when(is_end)
    def _():
        for d in range(1, 8):
            norm_copy(d).wait_send()


def settle(parts, *refs):
    w, hand, rest, results = refs[:3], (None, *refs[3:5]), refs[5:11], refs[11:20]
    slots, (in_sem, out_sem) = refs[20:24], refs[24:]
    me = lax.axis_index("dp")
    z, c = lax.div(me, 2), lax.rem(me, 2)
    is_inner = (z == 1) | (z == 2)
    items, used = [], [0] * 4

    def item(pool, src, dst, other=None, chosen=None):
        items.append((pool, used[pool] % slots[pool].shape[0], src, dst, other, chosen))
        used[pool] += 1

    for j in range(3):
        rows = w[j].shape[1] // (2 * CHIPS)
        for layer in range(LAYERS):
            for d in range(2 * CHIPS):
                at = (layer, pl.ds(d * rows, rows))
                handed = (hand[j].at[layer], is_inner & (d == (3 - z) * 2 + c)) if j else ()
                item(j // 2, w[j].at[at], results[j].at[at], *handed)
    for i in range(6):
        for layer in range(LAYERS):
            item(2 + i % 3 // 2, rest[i].at[layer], results[3 + i].at[layer])

    def get(t, src):
        pool, slot = items[t][:2]
        return pltpu.make_async_copy(src, slots[pool].at[slot], in_sem.at[pool, slot])

    def put(t):
        pool, slot, _, dst = items[t][:4]
        return pltpu.make_async_copy(slots[pool].at[slot], dst, out_sem.at[pool, slot])

    busy = {}
    for t in range(len(items) + parts):
        if t < len(items):
            pool, slot, src, _, other, chosen = items[t]
            if (pool, slot) in busy:
                put(busy.pop((pool, slot))).wait()
            if other is None:
                get(t, src).start()
            else:

                @pl.when(chosen)
                def _():
                    get(t, other).start()

                @pl.when(jnp.logical_not(chosen))
                def _():
                    get(t, src).start()

        if t >= parts:
            done = t - parts
            get(done, items[done][2]).wait()
            put(done).start()
            busy[items[done][:2]] = done
    for t in busy.values():
        put(t).wait()


def place(first, *refs):
    n = len(first)
    mine, others, results, buffers = (refs[i * n : (i + 1) * n] for i in (1, 2, 3, 4))
    in_sem, out_sem = refs[5 * n :]
    me = lax.axis_index("dp")
    z, c = lax.div(me, 2), lax.rem(me, 2)

    @pl.when((z == 0) | (z == 3))
    def _():
        chip = jnp.where(z == 0, 2, 1)
        gets, puts = [], []
        for j in range(n):
            layers, rows, _ = mine[j].shape
            for b, (src, core) in enumerate(((mine[j], c), (others[j], 1 - c))):
                for layer in range(layers):
                    at = pl.ds(pl.multiple_of((chip * 2 + core) * rows, rows), rows)
                    gets.append(pltpu.make_async_copy(src.at[layer], buffers[j].at[b, layer], in_sem.at[j, b, layer]))
                    puts.append(pltpu.make_async_copy(buffers[j].at[b, layer], results[j].at[first[j] + layer, at], out_sem.at[j, b, layer]))
        for copy in gets:
            copy.start()
        for get, put in zip(gets, puts, strict=True):
            get.wait()
            put.start()
        for copy in puts:
            copy.wait()


def solution(mesh):
    def step(*arrays):
        terms, weights, m, v = (arrays[i : i + 3] for i in (0, 3, 6, 9))
        terms = [t.reshape(t.shape[1:]) for t in terms]
        shapes = [one.shape for one in m]
        count = sum(t.size for t in terms)
        rs_total = sum(LAYERS * 2 * s[1] // r for s, r in zip(shapes, RS_ROWS, strict=True))
        ag_total = sum(LAYERS * s[1] // r for s, r in zip(shapes, AG_ROWS, strict=True))
        units = [pltpu.VMEM((LAYERS * CHIPS, s[1], s[2]), jnp.bfloat16) for s in shapes]
        wide, tall = shapes[0], shapes[2]

        def pair(slots, rows, dtype):
            return [pltpu.VMEM((*slots, rows[0], wide[2]), dtype), pltpu.VMEM((*slots, rows[2], tall[2]), dtype)]

        dma = pltpu.SemaphoreType.DMA
        outs = pl.pallas_call(
            lambda *refs: kernel(count, *refs),
            out_shape=[jax.ShapeDtypeStruct(one.shape, jnp.bfloat16) for one in weights]
            + [jax.ShapeDtypeStruct(one.shape, jnp.bfloat16) for one in m[1:]]
            + [jax.ShapeDtypeStruct(one.shape, jnp.float32) for one in (*m, *v)],
            in_specs=[pl.BlockSpec(memory_space=pl.ANY)] * 12,
            out_specs=[pl.BlockSpec(memory_space=pl.ANY)] * 11,
            scratch_shapes=units
            + units
            + pair((2, AHEAD + 1), RS_ROWS, jnp.bfloat16)
            + pair((READ + 1,), AG_ROWS, jnp.float32)
            + pair((READ + 1,), AG_ROWS, jnp.float32)
            + pair((READ + 1,), AG_ROWS, jnp.bfloat16)
            + pair((2,), AG_ROWS, jnp.float32)
            + pair((2,), AG_ROWS, jnp.float32)
            + [pltpu.VMEM((8, wide[2]), jnp.float32), pltpu.VMEM((8, tall[2]), jnp.float32)]
            + [pltpu.VMEM((8, 128), jnp.float32), pltpu.VMEM((4, 8, 128), jnp.float32)]
            + [
                dma((2, AHEAD + 1)),
                dma((3,)),
                dma((24,)),
                dma((2, 3)),
                dma((2, rs_total)),
                dma((7,)),
                dma((4,)),
                dma((3, READ + 1)),
                dma((2, 2)),
                dma((ag_total,)),
                dma((ag_total,)),
                dma((ag_total,)),
                dma((ag_total,)),
                dma((LAYERS * shapes[0][1] // AG_ROWS[0],)),
                dma((5, 3)),
                dma((3,)),
                dma((3,)),
                dma((3,)),
            ],
            name="clipped_step",
            compiler_params=pltpu.CompilerParams(collective_id=0, has_side_effects=True, vmem_limit_bytes=67043328),
        )(*terms, *weights, *m, *v)
        whole, hand, rest = outs[:3], outs[3:5], outs[5:]
        came = []
        for one in (hand[0], hand[1][:1], hand[1][1:]):
            came.append(lax.ppermute(one, "dp", [(2, 0), (3, 1), (4, 6), (5, 7)]))
        any_space = pl.BlockSpec(memory_space=pl.ANY)
        results = pl.pallas_call(
            lambda *refs: settle(4, *refs),
            out_shape=[jax.ShapeDtypeStruct(one.shape, one.dtype) for one in (*whole, *rest)],
            in_specs=[any_space] * 11,
            out_specs=[any_space] * 9,
            scratch_shapes=[
                pltpu.VMEM((8, *wide[1:]), jnp.bfloat16),
                pltpu.VMEM((8, *tall[1:]), jnp.bfloat16),
                pltpu.VMEM((6, *wide[1:]), jnp.float32),
                pltpu.VMEM((4, *tall[1:]), jnp.float32),
                dma((4, 8)),
                dma((4, 8)),
            ],
            name="settle",
            cost_estimate=pl.CostEstimate(flops=10**9, bytes_accessed=141 * 10**6, transcendentals=0),
            compiler_params=pltpu.CompilerParams(vmem_limit_bytes=62 * 2**20),
        )(*whole, *hand, *rest)
        others = []
        for j in range(3):
            came[j], _ = lax.optimization_barrier((came[j], results[3]))
            others.append(lax.ppermute(came[j], "dp", [(0, 1), (1, 0), (6, 7), (7, 6)]))

        def put(into, which, first):
            n = len(which)
            return pl.pallas_call(
                lambda *refs: place(first, *refs),
                out_shape=[jax.ShapeDtypeStruct(one.shape, one.dtype) for one in into],
                in_specs=[any_space] * (3 * n),
                out_specs=[any_space] * n,
                scratch_shapes=[pltpu.VMEM((2, *came[j].shape), jnp.bfloat16) for j in which] + [dma((n, 2, LAYERS)), dma((n, 2, LAYERS))],
                input_output_aliases={i: i for i in range(n)},
                name="place",
                cost_estimate=pl.CostEstimate(flops=10**7, bytes_accessed=n * 16 * 10**6, transcendentals=0),
            )(*into, *(came[j] for j in which), *(others[j] for j in which))

        up, down = put(results[1:3], (0, 1), (0, 0))
        (down,) = put([down], (2,), (1,))
        return (results[0], up, down, *results[3:])

    all_of, cut = P(None, None, None), P(None, "dp", None)
    return jax.shard_map(
        step,
        mesh=mesh,
        in_specs=(P(("rep", "dp"), None, None, None),) * 3 + (all_of,) * 3 + (cut,) * 6,
        out_specs=(P("rep", None, None),) * 3 + (P("rep", "dp", None),) * 6,
        check_vma=False,
    )
```
